32 devices in a mesh: groups: 2 (over x), dev: 16 (over z, y, core).
Axes of the slice: x: 2, y: 2, z: 4, core: 2. Of those that a mesh axis runs over, the one named last changes fastest.
Arguments:
- queries: bfloat16 [32, 512, 512], P(('groups', 'dev')), parts along dimension 0, may hold values from -120 to 120
- key_values: bfloat16 [2, 32, 512, 128], P(None, ('groups', 'dev')), parts along dimension 1, may hold values from -4 to 4
- lengths: int32 [4], P('groups'), parts along dimension 0, may hold values from 1 to 512, as said below
- out_proj: bfloat16 [4096, 2048], P('dev'), may hold values from -0.09375 to 0.09375
- residual: bfloat16 [32, 64, 2048], P(('groups', 'dev')), parts along dimension 0, may hold values from -8 to 8
- norm_gain: bfloat16 [2048], replicated, may hold values from 0.25 to 1.75
- router: bfloat16 [2048, 16], replicated, may hold values from -0.125 to 0.125
- expert_ids: int32 [32, 64, 8], P(('groups', 'dev')), parts along dimension 0, may hold values from 0 to 15, all different within a row; in each aligned block of 64 rows (0 to 63, 64 to 127, ..., all dimensions but the last counted through in order) at most 48 rows name the same one
- expert_gate_up: bfloat16 [16, 2048, 1536], P('dev'), may hold values from -0.125 to 0.125
- expert_down: bfloat16 [16, 768, 2048], P('dev'), may hold values from -0.21875 to 0.21875
Outputs:
- output: bfloat16 [32, 64, 2048], P(('groups', 'dev')), parts along dimension 0
The draws below stay inside these ranges and needn't reach their ends.
There are 2 independent parts, one for each index of `groups`. The reference program is written for one: setup_inputs(seed, part) draws one part's arguments, and reference() takes and returns one part's arrays. A program takes and returns all parts, laid end to end along the dimension named above; an argument that names none is the same for every part. Nothing has to cross between parts.
Inputs may be any that keep to these rules, and one draw needn't show every extreme that they name: `lengths`: in every draw some request has all 512 cache slots filled. Each token names 8 different experts. The tokens of one block of expert_ids name any one expert at most 48 times, and in every draw some block names some expert exactly 48 times.
All inputs are finite; a program needn't handle non-finite values.
Results may differ from the reference program's by a relative error of at most 0.011.
Values may be sent and summed in bfloat16 or wider, within the bound.
No kernel may reach another device: no remote copies, remote signals or barrier semaphores. Data moves between devices by JAX's collectives and lax.ppermute only.
A program may use at most 128 MiB of HBM per device.

```python
import math
import jax
import jax.numpy as jnp
import numpy as np
from jax import lax

D = 2048
HEADS = 32
KV_HEADS = 4
HEAD_DIM = 128
FF = 768
TOP = 8
TOK_DEV = 64
CTX = 512
GROUP = 8
QH = 4
REQS = 2
SPAN = 512
HALF = 512
EXPERTS = 16
CAP = 48


def attention_pair(key):
    base_key = jax.random.fold_in(key, 101)
    key_query, key_pairs = jax.random.split(base_key, 2)
    block_count = GROUP * REQS
    kv_draw = jnp.clip(jax.random.normal(key_pairs, (2, block_count, HALF, HEAD_DIM), jnp.float32), -4.0, 4.0)
    query_draw = jnp.clip(2.0 * jax.random.normal(key_query, (block_count, SPAN, QH * HEAD_DIM), jnp.float32), -8.0, 8.0)
    return (query_draw, kv_draw)


def draw_queries(key, part):
    return attention_pair(key)[0].astype(jnp.bfloat16)


def draw_key_values(key, part):
    return attention_pair(key)[1].astype(jnp.bfloat16)


def draw_lengths(key, part):
    base_key = jax.random.fold_in(key, 202)
    key_len, key_full = jax.random.split(base_key)
    drawn_len = jax.random.randint(key_len, (REQS,), 1, CTX)
    filled = jax.random.randint(key_full, (), 0, REQS)
    return jnp.where(jnp.arange(REQS) == filled, CTX, drawn_len).astype(jnp.int32)


def draw_residual(key, part):
    base_key = jax.random.fold_in(key, 303)
    key_noise = jax.random.fold_in(base_key, 0)
    noise_part = jax.random.normal(key_noise, (GROUP * REQS, TOK_DEV, D), jnp.float32)
    drawn_value = 0.25 * noise_part
    return jnp.clip(drawn_value, -8.0, 8.0).astype(jnp.bfloat16)


def steps_of(stream_key, dims, cuts, least, high):
    gain = 1.0
    for position, shards_of in cuts:
        steps = jax.random.uniform(jax.random.fold_in(jax.random.fold_in(stream_key, 6), position), (shards_of,), jnp.float32, least / len(cuts), high / len(cuts))
        gain = gain * jnp.repeat(jnp.exp(steps), dims[position] // shards_of).reshape((-1,) + (1,) * (len(dims) - 1 - position))
    return gain


def routed_block(stream_key, own, number, rows, amount, top, reach, slope):
    sequence = jax.random.permutation(stream_key, amount)
    packed, usual = load_shares(amount, rows * top, reach, slope, True), load_shares(amount, rows * top, reach, slope, False)
    places = jnp.arange(amount)

    def named(sizes, offset_by):
        used = int((sizes > 0).sum())
        fixed = max(1, used // 4)
        moved = fixed + (places - fixed + offset_by * (used - fixed)) % max(1, amount - fixed)
        return jnp.zeros((amount,), jnp.int32).at[sequence[jnp.where(places < fixed, places, moved)]].set(jnp.asarray(sizes, jnp.int32))

    sizes = jnp.where(number % 4 == 0, named(packed, number // 4), named(usual, number - number // 4 - 1))
    mixed = jax.random.permutation(jax.random.fold_in(own, 3), amount)
    source_of, taker = mixed[0:amount // 2 * 2:2], mixed[1:amount // 2 * 2:2]
    room = jnp.minimum(sizes[source_of] - 1, reach - sizes[taker]) // 2
    room = jnp.where((source_of == sequence[0]) | (taker == sequence[0]) | (sizes[taker] == 0), 0, jnp.maximum(room, 0))
    moved = jax.random.randint(jax.random.fold_in(own, 4), (amount // 2,), 0, 1 << 20) % (room + 1)
    sizes = sizes.at[source_of].add(-moved).at[taker].add(moved)
    items = jnp.searchsorted(jnp.cumsum(sizes), jnp.arange(rows * top), side="right").astype(jnp.int32)
    listing = items.reshape(top, rows).T
    listing = listing[jax.random.permutation(jax.random.fold_in(own, 1), rows)]
    offset_by = jax.random.randint(jax.random.fold_in(own, 2), (rows, 1), 0, top)
    return jnp.take_along_axis(listing, (jnp.arange(top)[None, :] + offset_by) % top, axis=1)


def load_shares(number_of, total, bound, skew, full):
    weights = [(1 << 20) // math.isqrt(standing ** skew) + 1 for standing in range(1, number_of + 1)]
    largest = bound if full else min(bound, max(-(-total // number_of), total * weights[0] // sum(weights)))
    least = 1 if total - largest >= number_of - 1 else 0
    given, spare = [largest] + [least] * (number_of - 1), total - largest - least * (number_of - 1)
    while spare > 0:
        free = [i for i in range(1, number_of) if given[i] < largest] or [i for i in range(1, number_of) if given[i] < bound]
        mass, left = sum([weights[i] for i in free]), spare
        for i in free:
            addition = min(bound - given[i], max(1, left * weights[i] // mass), spare)
            given[i] = given[i] + addition
            spare = spare - addition
    return np.array(given)


def noise(rng, extent, scale, reach, cuts=(), held_as=jnp.bfloat16):
    values = scale * jax.random.normal(rng, extent, jnp.float32)
    if cuts:
        values = values * steps_of(rng, extent, cuts, -0.22, 0.18)
    return jnp.clip(values, -reach, reach).astype(held_as)


def setup_inputs(seed: int = 0, part: int = 0) -> dict:
    arg_keys = jax.random.split(jax.random.key(seed), 11)
    part_splits = jax.random.split(jax.random.fold_in(arg_keys[10], part), 11)
    queries = draw_queries(jax.random.fold_in(jax.random.fold_in(arg_keys[10], part), 71), part)
    key_values = draw_key_values(jax.random.fold_in(jax.random.fold_in(arg_keys[10], part), 71), part)
    lengths = draw_lengths(jax.random.fold_in(jax.random.fold_in(arg_keys[10], part), 71), part)
    out_proj = noise(arg_keys[3], (HEADS * HEAD_DIM, D), (HEADS * HEAD_DIM) ** -0.5, 0.09375, ((0, 16),))
    residual = draw_residual(jax.random.fold_in(jax.random.fold_in(arg_keys[10], part), 71), part)
    norm_gain = jnp.clip(1.0 + 0.15 * jax.random.normal(arg_keys[5], (D,), jnp.float32), 0.25, 1.75).astype(jnp.bfloat16)
    router = noise(arg_keys[6], (D, EXPERTS), D ** -0.5, 0.125)
    expert_ids_keys = jax.random.split(jax.random.fold_in(part_splits[7], 1), (GROUP * REQS) * TOK_DEV // TOK_DEV)
    expert_ids_turns = jax.random.permutation(jax.random.fold_in(part_splits[7], 3), (GROUP * REQS) * TOK_DEV // TOK_DEV)
    expert_ids = jax.vmap(lambda own, number: routed_block(jax.random.fold_in(part_splits[7], 2), own, number, TOK_DEV, EXPERTS, TOP, CAP, 2))(expert_ids_keys, expert_ids_turns).reshape((GROUP * REQS, TOK_DEV, TOP))
    expert_gate_up = noise(arg_keys[8], (EXPERTS, D, 2 * FF), D ** -0.5, 0.125, ((0, 16),))
    expert_down = noise(arg_keys[9], (EXPERTS, FF, D), FF ** -0.5, 0.21875, ((0, 16),))
    return dict(queries=queries, key_values=key_values, lengths=lengths, out_proj=out_proj, residual=residual, norm_gain=norm_gain, router=router, expert_ids=expert_ids, expert_gate_up=expert_gate_up, expert_down=expert_down)


EPSILON = 1e-06

def route_slots(flat_ids):
    expert_marks = (flat_ids.reshape(-1)[:, None] == jnp.arange(EXPERTS, dtype=jnp.int32)[None, :]).astype(jnp.int32)
    before = jnp.cumsum(expert_marks, axis=0) - expert_marks
    return lax.optimization_barrier(jnp.sum(before * expert_marks, axis=1)).reshape(flat_ids.shape)

def slot_rows(flat_ids, slot_index):
    positions = (flat_ids * CAP + slot_index).reshape(-1).astype(jnp.int32)
    tokens = jnp.repeat(jnp.arange(TOK_DEV, dtype=jnp.int32), TOP)
    return jnp.full((EXPERTS * CAP,), -1, jnp.int32).at[positions].set(tokens)

def expert_rows(gathered, gate_up, down_proj):
    projected = jnp.dot(gathered, gate_up, preferred_element_type=jnp.float32)
    activation = (jax.nn.silu(projected[:, :FF]) * projected[:, FF:]).astype(jnp.bfloat16)
    return jnp.dot(activation, down_proj, preferred_element_type=jnp.float32).astype(jnp.bfloat16)

def reference(queries, key_values, lengths, out_proj, residual, norm_gain, router, expert_ids, expert_gate_up, expert_down):
    block_count = GROUP * REQS
    score_scale = 1.0 / math.sqrt(HEAD_DIM)
    kv_seq = key_values.reshape(2, KV_HEADS, 2, REQS, HALF, HEAD_DIM).transpose(0, 1, 3, 2, 4, 5)
    kv_seq = kv_seq.reshape(2, KV_HEADS, REQS, 2 * HALF, HEAD_DIM)
    query_blocks = queries.reshape(block_count, SPAN, QH, HEAD_DIM)
    positions = jnp.arange(CTX + SPAN, dtype=jnp.int32)
    row_ids = jnp.arange(SPAN, dtype=jnp.int32)
    rank_ids = jnp.arange(block_count, dtype=jnp.int32) // REQS
    requests = jnp.arange(block_count, dtype=jnp.int32) % REQS

    def attend(element):
        rank_no, request, block_q = element
        key_rows = kv_seq[0, rank_no // 2, request]
        value_rows = kv_seq[1, rank_no // 2, request]
        scores = jnp.einsum('tjd,pd->jtp', block_q.astype(jnp.float32), key_rows.astype(jnp.float32)) * score_scale
        visible = (positions[None, :] < lengths[request]) | (positions[None, :] >= CTX) & (positions[None, :] - CTX <= row_ids[:, None])
        scores = jnp.where(visible[None], scores, -jnp.inf)
        row_max = lax.optimization_barrier(jnp.max(scores, axis=-1, keepdims=True))
        raised = jnp.exp(scores - row_max)
        weights = (raised / lax.optimization_barrier(jnp.sum(raised, axis=-1, keepdims=True))).astype(jnp.bfloat16)
        mixture = jnp.einsum('jtp,pd->tjd', weights.astype(jnp.float32), value_rows.astype(jnp.float32))
        return mixture.astype(jnp.bfloat16)
    head_out = lax.map(attend, (rank_ids, requests, query_blocks))
    head_out = head_out.reshape(GROUP, REQS, SPAN, QH * HEAD_DIM).transpose(1, 2, 0, 3).reshape(REQS * SPAN, HEADS * HEAD_DIM)
    attended = jnp.dot(head_out, out_proj, preferred_element_type=jnp.float32)
    attended = attended.reshape(REQS, GROUP, TOK_DEV, D).transpose(1, 0, 2, 3).reshape(block_count, TOK_DEV, D)
    stream = (residual.astype(jnp.float32) + attended).astype(jnp.bfloat16)
    values = stream.astype(jnp.float32)
    normed = (values * lax.rsqrt(lax.optimization_barrier(jnp.mean(values * values, axis=-1, keepdims=True)) + EPSILON) * norm_gain.astype(jnp.float32)).astype(jnp.bfloat16)
    logits = jnp.dot(normed.reshape(block_count * TOK_DEV, D), router, preferred_element_type=jnp.float32).reshape(block_count, TOK_DEV, EXPERTS)
    onehot = expert_ids[..., None] == jnp.arange(EXPERTS, dtype=jnp.int32)
    chosen = lax.optimization_barrier(jnp.sum(jnp.where(onehot, logits[:, :, None, :], 0.0), axis=-1))
    raised_gate = jnp.exp(chosen)
    gate_weights = raised_gate / lax.optimization_barrier(jnp.sum(raised_gate, axis=-1, keepdims=True))
    slots = jax.vmap(route_slots)(expert_ids)
    slot_table = jax.vmap(slot_rows)(expert_ids, slots)

    def visit(summed, element):
        gate_up, down_proj, expert = element
        token_pick = lax.dynamic_slice_in_dim(slot_table, (expert * CAP).astype(jnp.int32), CAP, axis=1)
        gathered = jnp.take_along_axis(normed, jnp.maximum(token_pick, 0)[:, :, None], axis=1)
        outputs = expert_rows(gathered.reshape(block_count * CAP, D), gate_up, down_proj).reshape(block_count, CAP, D)
        is_chosen = expert_ids == expert
        weight = lax.optimization_barrier(jnp.sum(jnp.where(is_chosen, gate_weights, 0.0), axis=2))
        slot_pick = lax.optimization_barrier(jnp.sum(jnp.where(is_chosen, slots, 0), axis=2)).astype(jnp.int32)
        picked = jnp.take_along_axis(outputs, slot_pick[:, :, None], axis=1)
        return (summed + weight[:, :, None] * picked.astype(jnp.float32), None)
    summed, _ = lax.scan(visit, jnp.zeros((block_count, TOK_DEV, D), jnp.float32), (expert_gate_up, expert_down, jnp.arange(EXPERTS, dtype=jnp.int32)))
    return (values + summed).astype(jnp.bfloat16)
```

```python
import math

import jax
import jax.numpy as jnp
from jax import lax
from jax.sharding import PartitionSpec as P

HEAD_DIM = 128
GROUP = 8

EPSILON = 1e-06


def partner(block, axis, stride):
    count = lax.axis_size(axis)
    route = []
    for low in range(count):
        high = low | 1 << stride
        if high != low and high < count:
            route += [(low, high), (high, low)]
    return lax.ppermute(block, axis, route)


def bit_count(number):
    return number.bit_length() - 1


def attention(queries, key_seq, value_seq, length, ctx):
    span, width = queries.shape
    heads = width // HEAD_DIM
    positions = jnp.arange(key_seq.shape[0], dtype=jnp.int32)
    qblock = math.gcd(span, 256)
    score_scale = 1.0 / math.sqrt(HEAD_DIM)
    block_queries = queries.reshape(span // qblock, qblock, heads, HEAD_DIM)
    starts = jnp.arange(span // qblock, dtype=jnp.int32) * qblock

    def attend(element):
        block_q, start = element
        scores = (
            jnp.einsum("tjd,pd->jtp", block_q, key_seq, preferred_element_type=jnp.float32)
            * score_scale
        )
        row_ids = start + jnp.arange(qblock, dtype=jnp.int32)
        visible = (positions[None, :] < length) | (positions[None, :] >= ctx) & (
            positions[None, :] - ctx <= row_ids[:, None]
        )
        scores = jnp.where(visible[None], scores, -jnp.inf)
        row_max = jnp.max(scores, axis=-1, keepdims=True)
        raised = jnp.exp(scores - row_max)
        weights = (raised / jnp.sum(raised, axis=-1, keepdims=True)).astype(jnp.bfloat16)
        mixture = jnp.einsum("jtp,pd->tjd", weights, value_seq, preferred_element_type=jnp.float32)
        return mixture.astype(jnp.bfloat16)

    return lax.map(attend, (block_queries, starts)).reshape(span, width)


def per_device(
    queries,
    key_values,
    lengths,
    out_proj,
    residual,
    norm_gain,
    router,
    expert_ids,
    expert_gate_up,
    expert_down,
):
    devices = lax.axis_size("dev")
    my_index = lax.axis_index("dev")
    requests_n = devices // GROUP
    low_bits = bit_count(requests_n)
    rank_bits = bit_count(GROUP)
    pair_bit = low_bits
    line_bits = list(range(devices.bit_length() - 2, low_bits, -1))
    tp_rank = my_index // requests_n
    request = my_index % requests_n
    tok, width = residual.shape[1:]
    half = key_values.shape[2]
    own_half = key_values[:, 0]
    other_half = partner(own_half, "dev", pair_bit)
    is_upper = tp_rank % 2 == 1
    first_part = jnp.where(is_upper, other_half, own_half)
    second_part = jnp.where(is_upper, own_half, other_half)
    key_seq = jnp.concatenate([first_part, second_part], axis=1)
    head_out = attention(queries[0], key_seq[0], key_seq[1], lengths[request], half)

    proj_block = out_proj
    for bit_no in range(low_bits):
        arrived = partner(proj_block, "dev", bit_no)
        is_high = my_index >> bit_no & 1 == 1
        proj_block = jnp.where(
            is_high,
            jnp.concatenate([arrived, proj_block], axis=0),
            jnp.concatenate([proj_block, arrived], axis=0),
        )

    pieces = []
    for mask in range(GROUP):
        rows = lax.dynamic_slice_in_dim(head_out, (tp_rank ^ mask) * tok, tok, axis=0)
        pieces.append(rows)

    def project(group):
        stacked = jnp.concatenate(group, axis=0)
        return jnp.dot(stacked, proj_block, preferred_element_type=jnp.float32)

    line_parts = {}
    for line in range(GROUP // 2 - 1, -1, -1):
        both = project([pieces[2 * line], pieces[2 * line + 1]])
        arrived = partner(both[tok:].astype(jnp.bfloat16), "dev", pair_bit)
        line_parts[line] = both[:tok] + arrived.astype(jnp.float32)
    attended = reduce_line(line_parts, low_bits + 1, rank_bits - 1)

    stream = (residual[0].astype(jnp.float32) + attended).astype(jnp.bfloat16)
    values = stream.astype(jnp.float32)
    normed = (
        values
        * lax.rsqrt(jnp.mean(values * values, axis=-1, keepdims=True) + EPSILON)
        * norm_gain.astype(jnp.float32)
    ).astype(jnp.bfloat16)
    logits = jnp.dot(normed, router, preferred_element_type=jnp.float32)
    experts_n = router.shape[1]
    token_ids = expert_ids[0]
    chosen = jnp.any(token_ids[..., None] == jnp.arange(experts_n, dtype=jnp.int32), axis=1)
    raised = jnp.where(chosen, jnp.exp(logits), 0.0)
    gates = raised / jnp.sum(raised, axis=-1, keepdims=True)
    gates_high = lax.reduce_precision(gates, 8, 7)
    lanes = -(-2 * experts_n // 128) * 128
    tail = jnp.concatenate(
        [gates_high, gates - gates_high, jnp.zeros((tok, lanes - 2 * experts_n), jnp.float32)], axis=1
    ).astype(jnp.bfloat16)
    block = jnp.concatenate([normed, tail], axis=1)

    line_blocks = gather_line(block, low_bits + 1, rank_bits - 1)
    expert = my_index
    lane = jnp.arange(lanes, dtype=jnp.int32)
    mine = (lane == expert) | (lane == expert + experts_n)
    line_parts = {}
    for line in sorted(line_blocks):
        rows = line_blocks[line]
        rows = jnp.concatenate([rows, partner(rows, "dev", pair_bit)], axis=0)
        for bit_no in range(low_bits):
            rows = jnp.concatenate([rows, partner(rows, "dev", bit_no)], axis=0)
        gate = jnp.sum(
            jnp.where(mine, rows[:, width:].astype(jnp.float32), 0.0), axis=1, keepdims=True
        )
        projected = jnp.dot(
            rows[:, :width], expert_gate_up[0], preferred_element_type=jnp.float32
        )
        hidden = projected.shape[1] // 2
        activation = (jax.nn.silu(projected[:, :hidden]) * projected[:, hidden:]).astype(
            jnp.bfloat16
        )
        produced = jnp.dot(activation, expert_down[0], preferred_element_type=jnp.float32)
        produced = produced * gate
        for bit_no in [*range(low_bits - 1, -1, -1), pair_bit]:
            count = produced.shape[0] // 2
            arrived = partner(produced[count:].astype(jnp.bfloat16), "dev", bit_no)
            produced = produced[:count] + arrived.astype(jnp.float32)
        line_parts[line] = produced
    combined = reduce_line(line_parts, low_bits + 1, rank_bits - 1)
    return (values + combined).astype(jnp.bfloat16)[None]


def gather_line(block, first_bit, bits):
    found = {0: block}
    for bit_no in range(bits - 1, -1, -1):
        for mask in sorted(found):
            found[mask | 1 << bit_no] = partner(found[mask], "dev", first_bit + bit_no)
    return found


def reduce_line(parts, first_bit, bits):
    parts = dict(parts)
    for bit_no in range(bits):
        for mask in sorted(parts, reverse=True):
            if mask >> bit_no & 1:
                sent = parts.pop(mask).astype(jnp.bfloat16)
                arrived = partner(sent, "dev", first_bit + bit_no)
                parts[mask ^ 1 << bit_no] += arrived.astype(jnp.float32)
    return parts[0]


def solution(mesh):
    return jax.shard_map(
        per_device,
        mesh=mesh,
        in_specs=(
            P(("groups", "dev"), None, None),
            P(None, ("groups", "dev"), None, None),
            P("groups"),
            P("dev", None),
            P(("groups", "dev"), None, None),
            P(),
            P(),
            P(("groups", "dev"), None, None),
            P("dev", None, None),
            P("dev", None, None),
        ),
        out_specs=P(("groups", "dev"), None, None),
        check_vma=False,
    )
```
